32 devices in a mesh: groups: 2 (over y), cols: 4 (over z), rows: 4 (over x, core).
Axes of the slice: x: 2, y: 2, z: 4, core: 2. Of those that a mesh axis runs over, the one named last changes fastest.
Arguments:
- base_field: float32 [320, 64, 512], P(None, ('groups', 'cols'), 'rows'), parts along dimension 1, may hold values from -6 to 6
- control_field: float32 [320, 64, 512], P(None, ('groups', 'cols', 'rows')), parts along dimension 1, may hold values from -6 to 6
- first_kernel: bfloat16 [9, 320, 320], replicated, may hold values from -0.109375 to 0.109375
- second_kernel: bfloat16 [9, 320, 320], replicated, may hold values from -0.109375 to 0.109375
- control_kernel: bfloat16 [9, 320, 320], replicated, may hold values from -0.109375 to 0.109375
- first_bias: float32 [320], replicated, may hold values from -3 to 3
- second_bias: float32 [320], replicated, may hold values from -3 to 3
- control_bias: float32 [320], replicated, may hold values from -3 to 3
- to_control: bfloat16 [320, 320], replicated, may hold values from -0.3125 to 0.3125
- to_base: bfloat16 [320, 320], replicated, may hold values from -0.3125 to 0.3125
Outputs:
- base_out: float32 [320, 64, 512], P(None, ('groups', 'cols'), 'rows'), parts along dimension 1
- control_out: float32 [320, 64, 512], P(None, ('groups', 'cols', 'rows')), parts along dimension 1
The draws below stay inside these ranges and needn't reach their ends.
There are 2 independent parts, one for each index of `groups`. The reference program is written for one: setup_inputs(seed, part) draws one part's arguments, and reference() takes and returns one part's arrays. A program takes and returns all parts, laid end to end along the dimension named above; an argument that names none is the same for every part. Nothing has to cross between parts.
All inputs are finite; a program needn't handle non-finite values.
Results may differ from the reference program's by a relative error of at most 0.0033.
Values may be sent and summed in bfloat16 or wider, within the bound.
A program may use at most 64 MiB of HBM per device.

```python
import jax
import jax.numpy as jnp

C = 320
WIDTH = 32
HEIGHT = 512


def level_of(own_key, extent, shards, low, high):
    gain, own = 1.0, jax.random.fold_in(own_key, 6)
    for dim, blocks in shards:
        draws = jnp.exp(jax.random.uniform(jax.random.fold_in(own, dim), (blocks,), jnp.float32, low / len(shards), high / len(shards)))
        gain = gain * jnp.repeat(draws, extent[dim] // blocks).reshape([-1 if axis == dim else 1 for axis in range(len(extent))])
    return gain


def normal_values(stream_key, extent, scale, bound, shards=(), held_as=jnp.bfloat16):
    drawn = scale * jax.random.normal(stream_key, extent, jnp.float32)
    if shards:
        drawn = drawn * level_of(stream_key, extent, shards, -0.22, 0.18)
    return jnp.clip(drawn, -bound, bound).astype(held_as)


def setup_inputs(seed: int = 0, part: int = 0) -> dict:
    streams_of = jax.random.split(jax.random.key(seed), 11)
    part_splits = jax.random.split(jax.random.fold_in(streams_of[10], part), 11)
    return {
        "base_field": normal_values(part_splits[0], (C, WIDTH, HEIGHT), 1.0, 6.0, ((1, 4), (2, 4)), jnp.float32),
        "control_field": normal_values(part_splits[1], (C, WIDTH, HEIGHT), 1.0, 6.0, ((1, 16),), jnp.float32),
        "first_kernel": normal_values(streams_of[2], (9, C, C), (9 * C) ** -0.5, 0.109375),
        "second_kernel": normal_values(streams_of[3], (9, C, C), (9 * C) ** -0.5, 0.109375),
        "control_kernel": normal_values(streams_of[4], (9, C, C), (9 * C) ** -0.5, 0.109375),
        "first_bias": normal_values(streams_of[5], (C,), 0.5, 3.0, (), jnp.float32),
        "second_bias": normal_values(streams_of[6], (C,), 0.5, 3.0, (), jnp.float32),
        "control_bias": normal_values(streams_of[7], (C,), 0.5, 3.0, (), jnp.float32),
        "to_control": normal_values(streams_of[8], (C, C), C ** -0.5, 0.3125),
        "to_base": normal_values(streams_of[9], (C, C), C ** -0.5, 0.3125),
    }


def convolve(field, weight, bias):
    padded = jnp.pad(field, ((0, 0), (1, 1), (1, 1))).astype(jnp.float32)
    width = field.shape[1]
    height = field.shape[2]
    total = jnp.zeros((weight.shape[1], width, height), jnp.float32)
    for offset in range(9):
        across = offset // 3
        down = offset % 3
        window = padded[:, across:across + width, down:down + height]
        total = total + jnp.einsum("oc,cwh->owh", weight[offset].astype(jnp.float32), window)
    return total + bias[:, None, None]


def project(matrix, field):
    return jnp.einsum("oc,cwh->owh", matrix.astype(jnp.float32), field.astype(jnp.float32))


def reference(base_field, control_field, first_kernel, second_kernel, control_kernel, first_bias, second_bias, control_bias, to_control, to_base):
    base_round = base_field.astype(jnp.bfloat16)
    hidden = jax.nn.silu(convolve(base_round, first_kernel, first_bias)).astype(jnp.bfloat16)
    base_mid = jax.nn.silu(convolve(hidden, second_kernel, second_bias)) + base_field
    control_round = control_field.astype(jnp.bfloat16)
    control_mid = jax.nn.silu(convolve(control_round, control_kernel, control_bias)) + control_field
    control_out = control_mid + project(to_control, base_mid.astype(jnp.bfloat16))
    base_out = base_mid + project(to_base, control_out.astype(jnp.bfloat16))
    return base_out, control_out
```

```python
import functools

import jax
import jax.numpy as jnp
from jax import lax
from jax.experimental import pallas as pl
from jax.experimental.pallas import tpu as pltpu
from jax.sharding import PartitionSpec as P

MESH = pl.DeviceIdType.MESH
BF = jnp.bfloat16
F32 = jnp.float32
LANE = 128
PACK = 16
SIDES = ((-1, 0), (1, 0), (0, -1), (0, 1), (-1, -1), (1, -1), (-1, 1), (1, 1))


def silu(v):
    return 0.5 * v * (1.0 + jnp.tanh(0.5 * v))


def kernel(
    n_cols,
    n_rows,
    base_hbm,
    control_hbm,
    k1_hbm,
    k2_hbm,
    kc_hbm,
    b1_ref,
    b2_ref,
    bc_ref,
    tc_ref,
    tb_ref,
    base_out,
    control_out,
    base,
    control,
    raw,
    packed,
    shifts_b,
    shifts_h,
    shifts_c,
    biases,
    edge_out,
    edge_in,
    strips,
    mid,
    result,
    bracket,
    arrived,
    load_sem,
    x_send,
    x_recv,
    in_send,
    in_recv,
    out_send,
    out_recv,
):
    C = base.shape[0]
    tile_cols = base.shape[1]
    strip_cols = control.shape[1]
    wide = strip_cols * LANE
    main = C - C % LANE
    rest = C - main
    full = packed.shape[1] - C
    gid = lax.axis_index("groups")
    k = lax.axis_index("cols")
    r = lax.axis_index("rows")
    lane = lax.broadcasted_iota(jnp.int32, (C, LANE), 1)

    loads = []
    for i, (src, dst) in enumerate(
        (
            (base_hbm, base),
            (control_hbm, control),
            (k1_hbm, raw.at[0]),
            (k2_hbm, raw.at[1]),
            (kc_hbm, raw.at[2]),
        )
    ):
        copy = pltpu.make_async_copy(src, dst, load_sem.at[i])
        copy.start()
        loads.append(copy)

    def there(side):
        dk, dr = side
        ok = None
        for at, step, count in ((k, dk, n_cols), (r, dr, n_rows)):
            if step:
                test = (at > 0) if step < 0 else (at < count - 1)
                ok = test if ok is None else jnp.logical_and(ok, test)
        return ok

    def partner(o):
        if n_rows & (n_rows - 1):
            return lax.rem(r + o, n_rows), lax.rem(r + n_rows - o, n_rows)
        q, bit = r, 1
        while bit < n_rows:
            if o & bit:
                q = q + bit * (1 - 2 * lax.rem(lax.div(r, bit), 2))
            bit *= 2
        return q, q

    order = [o for o in range(n_rows // 2, n_rows)] + [o for o in range(1, n_rows // 2)]

    barrier = pltpu.get_barrier_semaphore()
    peers = n_rows - 1
    for side in SIDES:
        if side[0]:
            peers = peers + jnp.where(there(side), 1, 0)

            @pl.when(there(side))
            def _():
                pl.semaphore_signal(
                    barrier, inc=1, device_id=(gid, k + side[0], r + side[1]), device_id_type=MESH
                )
    for o in order:
        pl.semaphore_signal(barrier, inc=1, device_id=(gid, k, partner(o)[0]), device_id_type=MESH)

    def entered():
        pl.semaphore_wait(barrier, peers)

    def slot(s, count=1):
        return pl.ds(s * LANE, count * LANE)

    blocks = {(0, -1): 0, (-1, -1): 1, (1, -1): 2, (0, 1): 3, (-1, 1): 4, (1, 1): 5}

    def exchange(index, shifts):
        made = []
        for i, side in enumerate(SIDES):
            dk, dr = side
            if dr == 0:
                src = shifts.at[1, :, slot(1 if dk < 0 else tile_cols)]
                dst = shifts.at[1, :, slot(tile_cols + 1 if dk < 0 else 0)]
            else:
                src = edge_out.at[index, pl.ds(0 if dr < 0 else PACK, PACK), :]
                dst = edge_in.at[index, pl.ds(PACK * blocks[(-dk, -dr)], PACK), :]
            made.append(
                pltpu.make_async_remote_copy(
                    src_ref=src,
                    dst_ref=dst,
                    send_sem=x_send.at[index, i],
                    recv_sem=x_recv.at[index, i],
                    device_id=(gid, k + dk, r + dr),
                    device_id_type=MESH,
                )
            )
        return made

    def opposite(i):
        return SIDES.index((-SIDES[i][0], -SIDES[i][1]))

    def send_edges(index, shifts):
        made = exchange(index, shifts)
        for i in (3, 2, 0, 1, 4, 5, 6, 7):
            @pl.when(there(SIDES[i]))
            def _():
                made[i].start()

    def await_edges(index, shifts):
        made = exchange(index, shifts)
        for i, side in enumerate(SIDES):
            @pl.when(there(side))
            def _():
                made[opposite(i)].wait_recv()

    def await_sent(index, shifts):
        made = exchange(index, shifts)
        for i, side in enumerate(SIDES):
            @pl.when(there(side))
            def _():
                made[i].wait_send()

    def clear_edges(index, shifts):
        for side in SIDES:
            dk, dr = side

            @pl.when(jnp.logical_not(there(side)))
            def _():
                if dr == 0:
                    shifts[1, :, slot(0 if dk < 0 else tile_cols + 1)] = jnp.zeros((C, LANE), BF)
                else:
                    edge_in[index, pl.ds(PACK * blocks[side], PACK), :] = jnp.zeros(
                        (PACK, edge_in.shape[2]), BF
                    )

    def pack_column(edges, w, value):
        edges = jnp.where(lane == w + 1, value[:, 0:1], edges)
        return jnp.where(lane == PACK + w + 1, value[:, LANE - 1 : LANE], edges)

    def store_edges(index, edges):
        spare = edge_out.shape[2] - C
        tall = jnp.concatenate([edges, jnp.zeros((spare, LANE), F32)], axis=0)
        edge_out[index] = tall.T[: 2 * PACK].astype(BF)

    def make_shifts(index, shifts):
        halo = edge_in[index].astype(F32).T[:C]
        for s in range(tile_cols + 2):
            if s == 0:
                at = PACK + tile_cols
            elif s == tile_cols + 1:
                at = 2 * PACK + 1
            else:
                at = s
            value = shifts[1, :, slot(s)].astype(F32)
            before = jnp.where(lane == 0, halo[:, at : at + 1], pltpu.roll(value, 1, 1))
            at += 3 * PACK
            after = jnp.where(
                lane == LANE - 1, halo[:, at : at + 1], pltpu.roll(value, LANE - 1, 1)
            )
            shifts[0, :, slot(s)] = before.astype(BF)
            shifts[2, :, slot(s)] = after.astype(BF)

    def pack_weights(i):
        loads[2 + i].wait()
        for t in range(9):
            packed[i, :, pl.ds(t * main, main)] = raw[i, t, :, :main]
        for t in range(0, 9, 2):
            here = raw[i, t, :, main:]
            at = 9 * main + t * rest
            if t < 8:
                here = jnp.concatenate([here, raw[i, t + 1, :, main:]], axis=1)
            packed[i, :, pl.ds(at, here.shape[1])] = here

    def convolve(i, shifts, q):
        pieces, last = [], []
        for t in range(9):
            at = pl.ds(pl.multiple_of((q * strip_cols + t // 3) * LANE, LANE), wide)
            pieces.append(shifts[t % 3, :main, at])
            last.append(shifts[t % 3, main:, at])
        patch = jnp.concatenate(pieces + last, axis=0)
        total = jnp.dot(packed[i], patch, preferred_element_type=F32)
        return total + jnp.concatenate([biases[i]] * strip_cols, axis=1)

    def part(q):
        return pl.ds(pl.multiple_of(q * wide, LANE), wide)

    def inner(q):
        return pl.ds(pl.multiple_of(q * wide + LANE, LANE), wide)

    loads[0].wait()
    edges = jnp.zeros((C, LANE), F32)
    for w in range(tile_cols):
        value = base[:, w, :].astype(BF)
        shifts_b[1, :, slot(w + 1)] = value
        edges = pack_column(edges, w, value.astype(F32))
    store_edges(0, edges)
    entered()
    send_edges(0, shifts_b)

    loads[1].wait()
    for q in range(n_rows):
        strips[q] = jnp.concatenate(
            [control[:, w, pl.ds(q * LANE, LANE)] for w in range(strip_cols)], axis=1
        ).astype(BF)

    def to_tile(j, o):
        q, _ = partner(o)
        return pltpu.make_async_remote_copy(
            src_ref=strips.at[q],
            dst_ref=shifts_c.at[1, :, inner(r)],
            send_sem=in_send.at[j],
            recv_sem=in_recv.at[j],
            device_id=(gid, k, q),
            device_id_type=MESH,
        )

    def to_strip(j, o):
        q, _ = partner(o)
        return pltpu.make_async_remote_copy(
            src_ref=bracket.at[q],
            dst_ref=arrived.at[r],
            send_sem=out_send.at[j],
            recv_sem=out_recv.at[j],
            device_id=(gid, k, q),
            device_id_type=MESH,
        )

    for j, o in enumerate(order):
        to_tile(j, o).start()
    shifts_c[1, :, inner(r)] = strips[r]

    for i, (index, ref) in enumerate(((0, b1_ref), (1, b2_ref), (2, bc_ref))):
        row = jnp.concatenate([ref[...], jnp.zeros((1, edge_out.shape[2] - C), F32)], axis=1)
        biases[i] = jnp.broadcast_to(row, (LANE, edge_out.shape[2])).T[:C]
    for index, shifts in enumerate((shifts_b, shifts_h, shifts_c)):
        clear_edges(index, shifts)
    pack_weights(0)

    await_edges(0, shifts_b)
    make_shifts(0, shifts_b)
    edges = jnp.zeros((C, LANE), F32)
    for q in range(n_rows):
        value = silu(convolve(0, shifts_b, q)).astype(BF)
        shifts_h[1, :, pl.ds(q * wide + LANE, wide)] = value
        for w in range(strip_cols):
            edges = pack_column(
                edges, q * strip_cols + w, value[:, w * LANE : (w + 1) * LANE].astype(F32)
            )
    store_edges(1, edges)
    send_edges(1, shifts_h)
    pack_weights(1)
    pack_weights(2)

    for j, o in enumerate(order):
        to_tile(j, o).wait_recv()
    edges = jnp.zeros((C, LANE), F32)
    for w in range(tile_cols):
        edges = pack_column(edges, w, shifts_c[1, :, slot(w + 1)].astype(F32))
    store_edges(2, edges)
    send_edges(2, shifts_c)

    await_edges(1, shifts_h)
    make_shifts(1, shifts_h)
    for q in range(n_rows):
        own = jnp.concatenate([base[:, q * strip_cols + w, :] for w in range(strip_cols)], axis=1)
        mid[:, pl.ds(q * wide, wide)] = silu(convolve(1, shifts_h, q)) + own

    await_edges(2, shifts_c)
    make_shifts(2, shifts_c)
    for j, o in enumerate(order + [0]):
        q = partner(o)[0] if o else r
        here = mid[:, part(q)]
        change = silu(convolve(2, shifts_c, q)) + jnp.dot(
            tc_ref[...], here.astype(BF), preferred_element_type=F32
        )
        bracket[q] = change.astype(BF)
        if o:
            to_strip(j, o).start()
        send = (change + shifts_c[1, :, inner(q)].astype(F32)).astype(BF)
        result[:, part(q)] = here + jnp.dot(tb_ref[...], send, preferred_element_type=F32)
    arrived[r] = bracket[r]

    for w in range(tile_cols):
        base_out[:, w, :] = result[:, slot(w)]
    for j, o in enumerate(order):
        to_strip(j, o).wait_recv()
    for q in range(n_rows):
        for w in range(strip_cols):
            at = pl.ds(q * LANE, LANE)
            control_out[:, w, at] = control[:, w, at] + arrived[q, :, slot(w)].astype(F32)
    for index, shifts in enumerate((shifts_b, shifts_h, shifts_c)):
        await_sent(index, shifts)
    for j, o in enumerate(order):
        to_tile(j, o).wait_send()
        to_strip(j, o).wait_send()


def solution(mesh):
    n_cols, n_rows = mesh.shape["cols"], mesh.shape["rows"]

    def per_device(base, control, k1, k2, kc, b1, b2, bc, tc, tb):
        C, tile_cols, _ = base.shape
        strip_cols = control.shape[1]
        wide = strip_cols * LANE
        tall = -(-C // LANE) * LANE
        area = tile_cols * LANE
        held = pltpu.VMEM((3, C, area + 2 * LANE), BF)
        others = n_rows - 1
        any_spec = pl.BlockSpec(memory_space=pl.ANY)
        vmem = pl.BlockSpec(memory_space=pltpu.VMEM)
        return pl.pallas_call(
            functools.partial(kernel, n_cols, n_rows),
            out_shape=(
                jax.ShapeDtypeStruct(base.shape, F32),
                jax.ShapeDtypeStruct(control.shape, F32),
            ),
            in_specs=[any_spec] * 5 + [vmem] * 5,
            out_specs=(vmem, vmem),
            scratch_shapes=[
                pltpu.VMEM(base.shape, F32),
                pltpu.VMEM(control.shape, F32),
                pltpu.VMEM((3,) + k1.shape, BF),
                pltpu.VMEM((3, C, 9 * C), BF),
                held,
                held,
                held,
                pltpu.VMEM((3, C, LANE), F32),
                pltpu.VMEM((3, 2 * PACK, tall), BF),
                pltpu.VMEM((3, LANE, tall), BF),
                pltpu.VMEM((n_rows, C, wide), BF),
                pltpu.VMEM((C, area), F32),
                pltpu.VMEM((C, area), F32),
                pltpu.VMEM((n_rows, C, wide), BF),
                pltpu.VMEM((n_rows, C, wide), BF),
                pltpu.SemaphoreType.DMA((5,)),
                pltpu.SemaphoreType.DMA((3, 8)),
                pltpu.SemaphoreType.DMA((3, 8)),
                pltpu.SemaphoreType.DMA((others,)),
                pltpu.SemaphoreType.DMA((others,)),
                pltpu.SemaphoreType.DMA((others,)),
                pltpu.SemaphoreType.DMA((others,)),
            ],
            compiler_params=pltpu.CompilerParams(
                collective_id=0, has_side_effects=True, vmem_limit_bytes=60 * 1024 * 1024
            ),
        )(base, control, k1, k2, kc, b1[None], b2[None], bc[None], tc, tb)

    tiles = P(None, ("groups", "cols"), "rows")
    lines = P(None, ("groups", "cols", "rows"), None)
    return jax.shard_map(
        per_device,
        mesh=mesh,
        in_specs=(tiles, lines) + (P(),) * 8,
        out_specs=(tiles, lines),
        check_vma=False,
    )
```
